32 devices in a mesh: dp: 4 (over z), ctx: 4 (over y, core), tp: 2 (over x).
Axes of the slice: x: 2, y: 2, z: 4, core: 2. Of those that a mesh axis runs over, the one named last changes fastest.
Arguments:
- hidden: bfloat16 [4, 512, 4096], P('dp', 'ctx'), may hold values from -6 to 6
- query_heads: bfloat16 [4, 512, 4096], P('dp', 'ctx', 'tp'), may hold values from -6 to 6
- key_heads: bfloat16 [4, 512, 512], P('dp', 'ctx', 'tp'), may hold values from -6 to 6
- value_heads: bfloat16 [4, 512, 512], P('dp', 'ctx', 'tp'), may hold values from -6 to 6
- attention_out: bfloat16 [4, 512, 4096], P('dp', 'ctx', 'tp'), may hold values from -3 to 3
- output_grad: bfloat16 [4, 512, 4096], P('dp', 'ctx', 'tp'), may hold values from -3 to 3
- log_norm: float32 [4, 32, 512], P('dp', 'tp', 'ctx'), may hold values from -40 to 40, as said below
- block_order: int32 [8], replicated, may hold values from 0 to 7, as said below
- value_weight: bfloat16 [4096, 512], P(None, 'tp'), may hold values from -0.25 to 0.25
Outputs:
- query_grad: bfloat16 [4, 512, 4096], P('dp', 'ctx', 'tp')
- key_grad: bfloat16 [4, 512, 512], P('dp', 'ctx', 'tp')
- value_grad: bfloat16 [4, 512, 512], P('dp', 'ctx', 'tp')
- hidden_grad: bfloat16 [4, 512, 4096], P('dp', 'ctx', 'tp')
- weight_grad: float32 [4096, 512], P('ctx', 'tp')
The draws below stay inside these ranges and needn't reach their ends.
Inputs may be any that keep to these rules, and one draw needn't show every extreme that they name: `block_order`: each of 0 to 7 once. log_norm is the log of the sum of exp(scores) over the keys visible to that row, so the probabilities of each row and head sum to one.
All inputs are finite; a program needn't handle non-finite values.
Results may differ from the reference program's by a relative error of at most 0.025.
Values may be sent and summed in bfloat16 or wider, within the bound.
No kernel may reach another device: no remote copies, remote signals or barrier semaphores. Data moves between devices by JAX's collectives and lax.ppermute only.
A program may use at most 64 MiB of HBM per device.

```python
import jax
import jax.numpy as jnp
from jax import lax

D = 4096
HD = 128
HQ = 32
KVH = 4
TOK_DEV = 128
SEQS = 4
LEN = 512
BLK = 64
NBLK = 8
N_CTX = 4


def attention_inputs(key):
    block_perm = jax.random.permutation(jax.random.fold_in(key, 501), NBLK).astype(jnp.int32)
    query_shape = (SEQS, LEN, HQ * HD)
    key_shape = (SEQS, LEN, KVH * HD)
    query_vals = jax.random.truncated_normal(jax.random.fold_in(key, 502), -6.0, 6.0, query_shape, jnp.float32)
    key_vals = jax.random.truncated_normal(jax.random.fold_in(key, 503), -6.0, 6.0, key_shape, jnp.float32)
    return (block_perm, query_vals.astype(jnp.bfloat16), key_vals.astype(jnp.bfloat16))


def draw_block_order(key, part):
    block_perm, query_vals, key_vals = attention_inputs(key)
    return block_perm


def draw_query_heads(key, part):
    block_perm, query_vals, key_vals = attention_inputs(key)
    return query_vals


def draw_key_heads(key, part):
    block_perm, query_vals, key_vals = attention_inputs(key)
    return key_vals


def draw_log_norm(key, part):
    block_perm, query_vals, key_vals = attention_inputs(key)
    row_ids = jnp.arange(LEN, dtype=jnp.int32)
    positions = block_perm[row_ids // BLK] * BLK + row_ids % BLK
    visible = positions[None, :] <= positions[:, None]
    members = HQ // KVH
    grouped = query_vals.astype(jnp.float32).reshape(SEQS, LEN, KVH, members, HD).transpose(0, 2, 3, 1, 4).reshape(SEQS * KVH, members, LEN, HD)
    keyed = key_vals.astype(jnp.float32).reshape(SEQS, LEN, KVH, HD).transpose(0, 2, 1, 3).reshape(SEQS * KVH, LEN, HD)

    def normalizer(pair):
        scores = jnp.einsum('jte,ke->jtk', pair[0], pair[1]) * HD ** (-0.5)
        return jax.scipy.special.logsumexp(jnp.where(visible[None], scores, -jnp.inf), axis=-1)
    return lax.map(normalizer, (grouped, keyed)).reshape(SEQS, HQ, LEN)


def strengthened(result, key, source, target, shards_of, factor):
    def block_of(dim):
        return (jnp.arange(result.shape[dim]) // (result.shape[dim] // shards_of)).reshape((-1,) + (1,) * (result.ndim - 1 - dim))

    near = jax.random.permutation(key, shards_of)[block_of(target)]
    second = (block_of(target) + shards_of // 2) % shards_of
    return jnp.where((block_of(source) == near) | (block_of(source) == second), factor * result, result)


def shard_levels(rng, extent, pieces, least, high):
    def one(dim, blocks):
        heights = jax.random.uniform(jax.random.fold_in(jax.random.fold_in(rng, 6), dim), (blocks,), jnp.float32, least / len(pieces), high / len(pieces))
        return jnp.repeat(jnp.exp(heights), extent[dim] // blocks).reshape((-1,) + (1,) * (len(extent) - dim - 1))

    loudness = one(*pieces[0])
    for cut in pieces[1:]:
        loudness = loudness * one(*cut)
    return loudness


def centred(stream_key, shape, spread, reach, pieces=(), kind=jnp.bfloat16):
    loudness = shard_levels(stream_key, shape, pieces, -0.22, 0.18) if pieces else 1.0
    drawn = jax.random.normal(stream_key, shape, jnp.float32) * spread * loudness
    return jnp.minimum(jnp.maximum(drawn, -reach), reach).astype(kind)


def bell_draw_with(own_key, extent, spread, reach, cuts, heavy, kind=jnp.bfloat16):
    values = spread * jax.random.normal(own_key, extent, jnp.float32)
    if cuts:
        values = values * shard_levels(own_key, extent, cuts, -0.22, 0.18)
    return jnp.clip(strengthened(values, jax.random.fold_in(own_key, 3), *heavy), -reach, reach).astype(kind)


def setup_inputs(seed: int = 0) -> dict:
    arg_keys = jax.random.split(jax.random.key(seed), 10)
    return {
        "hidden": bell_draw_with(arg_keys[0], (SEQS, LEN, D), 1.0, 6.0, ((0, 4), (1, 4)), (1, 2, 4, 2.0)),
        "query_heads": draw_query_heads(jax.random.fold_in(arg_keys[9], 71), 0),
        "key_heads": draw_key_heads(jax.random.fold_in(arg_keys[9], 71), 0),
        "value_heads": centred(arg_keys[3], (SEQS, LEN, KVH * HD), 1.0, 6.0, ((0, 4), (1, 4), (2, 2))),
        "attention_out": centred(arg_keys[4], (SEQS, LEN, HQ * HD), 0.5, 3.0, ((0, 4), (1, 4), (2, 2))),
        "output_grad": centred(arg_keys[5], (SEQS, LEN, HQ * HD), 0.5, 3.0, ((0, 4), (1, 4), (2, 2))),
        "log_norm": draw_log_norm(jax.random.fold_in(arg_keys[9], 71), 0),
        "block_order": draw_block_order(jax.random.fold_in(arg_keys[9], 71), 0),
        "value_weight": centred(arg_keys[8], (D, KVH * HD), (KVH * HD) ** -0.5, 0.25, ((1, 2),)),
    }


def storage_positions(block_order):
    row_ids = jnp.arange(LEN, dtype=jnp.int32)
    return block_order[row_ids // BLK] * BLK + row_ids % BLK


def reference(hidden, query_heads, key_heads, value_heads, attention_out, output_grad, log_norm, block_order, value_weight):
    positions = storage_positions(block_order)
    visible = positions[None, :] <= positions[:, None]
    members = HQ // KVH
    score_scale = HD ** -0.5

    def by_group(array):
        return array.astype(jnp.float32).reshape(SEQS, LEN, KVH, members, HD).transpose(0, 2, 3, 1, 4).reshape(SEQS * KVH, members, LEN, HD)

    def by_head(array):
        return array.astype(jnp.float32).reshape(SEQS, LEN, KVH, HD).transpose(0, 2, 1, 3).reshape(SEQS * KVH, LEN, HD)

    def pair_grads(items):
        queries, keys_f, values_f, outs_f, grads_f, norms_f = items
        scores = jnp.einsum('jte,ke->jtk', queries, keys_f) * score_scale
        probability = jnp.exp(jnp.where(visible[None], scores - norms_f[:, :, None], -jnp.inf))
        weights = lax.optimization_barrier(probability.astype(jnp.bfloat16)).astype(jnp.float32)
        row_delta = jnp.sum(grads_f * outs_f, axis=-1)
        value_part = jnp.einsum('jtk,jte->ke', weights, grads_f)
        through = jnp.einsum('jte,ke->jtk', grads_f, values_f)
        slopes = lax.optimization_barrier((probability * (through - row_delta[:, :, None])).astype(jnp.bfloat16)).astype(jnp.float32)
        query_part = score_scale * jnp.einsum('jtk,ke->jte', slopes, keys_f)
        key_part = score_scale * jnp.einsum('jtk,jte->ke', slopes, queries)
        return query_part, key_part, value_part

    query_parts, key_parts, value_parts = lax.map(pair_grads, (by_group(query_heads), by_head(key_heads), by_head(value_heads), by_group(attention_out), by_group(output_grad), log_norm.reshape(SEQS * KVH, members, LEN)))
    query_grad = query_parts.reshape(SEQS, KVH, members, LEN, HD).transpose(0, 3, 1, 2, 4).reshape(SEQS, LEN, HQ * HD).astype(jnp.bfloat16)
    key_grad = key_parts.reshape(SEQS, KVH, LEN, HD).transpose(0, 2, 1, 3).reshape(SEQS, LEN, KVH * HD).astype(jnp.bfloat16)
    value_grad = value_parts.reshape(SEQS, KVH, LEN, HD).transpose(0, 2, 1, 3).reshape(SEQS, LEN, KVH * HD).astype(jnp.bfloat16)
    flat_value = value_grad.reshape(SEQS * LEN, KVH * HD)
    hidden_grad = jnp.dot(flat_value, value_weight.T, preferred_element_type=jnp.float32).astype(jnp.bfloat16).reshape(SEQS, LEN, D)
    pieces_in = hidden.reshape(SEQS * N_CTX, TOK_DEV, D)
    pieces_grad = value_grad.reshape(SEQS * N_CTX, TOK_DEV, KVH * HD)

    def add_piece(summed, pair):
        partial_value = jnp.dot(pair[0].T, pair[1], preferred_element_type=jnp.float32)
        rounded = lax.optimization_barrier(partial_value.astype(jnp.bfloat16))
        return summed + rounded.astype(jnp.float32), None

    summed, unused = lax.scan(add_piece, jnp.zeros((D, KVH * HD), jnp.float32), (pieces_in, pieces_grad))
    weight_grad = summed * (SEQS * LEN) ** -0.5
    return query_grad, key_grad, value_grad, hidden_grad, weight_grad
```

```python
import jax
import jax.numpy as jnp
from jax import lax
from jax.experimental import pallas as pl
from jax.experimental.pallas import tpu as pltpu
from jax.sharding import PartitionSpec as P

HD = 128
HQ = 32
KVH = 4
F32 = jnp.float32
BF16 = jnp.bfloat16
NT = (((1,), (1,)), ((), ()))
NN = (((1,), (0,)), ((), ()))


def is_pow2(n):
    return n & (n - 1) == 0


def swap(x, axis, s):
    n = lax.axis_size(axis)
    return lax.ppermute(x, axis, [(i, i ^ s) for i in range(n)])


def probability(meta, q_pair, norm_pair, key_ref, s, tokens):
    rank = meta[0]
    block = tokens // 2
    lane = lax.broadcasted_iota(jnp.int32, (1, 2 * tokens), 1) % tokens
    q_first = jnp.where(lane < block, meta[1 + 2 * rank], meta[2 + 2 * rank])
    q_pos = q_first * block + lane % block
    owner = rank ^ s
    row = lax.broadcasted_iota(jnp.int32, (tokens, 1), 0)
    k_first = jnp.where(row < block, meta[1 + 2 * owner], meta[2 + 2 * owner])
    k_pos = k_first * block + row % block
    scores = lax.dot_general(key_ref[0], q_pair, NT, preferred_element_type=F32)
    shifted = scores * (HD ** (-0.5)) - norm_pair
    return jnp.exp(jnp.where(k_pos <= q_pos, shifted, -jnp.inf))


def pair_of(ref, h):
    return jnp.concatenate(
        [ref[0, :, h * HD : (h + 1) * HD], ref[0, :, (h + 1) * HD : (h + 2) * HD]], axis=0
    )


def rows_of(ref, h):
    return jnp.concatenate([ref[0, h : h + 1, :], ref[0, h + 1 : h + 2, :]], axis=1)


def value_kernel(n, members, tokens, meta, q_ref, g_ref, norm_ref, *rest):
    keys, out_ref, weights = rest[:n], rest[n], rest[n + 1]
    g_all = jnp.concatenate([g_ref[0, :, h * HD : (h + 1) * HD] for h in range(members)], axis=0)
    for h in range(0, members, 2):
        q_pair = pair_of(q_ref, h)
        norm_pair = rows_of(norm_ref, h)
        for s in range(n):
            p = probability(meta, q_pair, norm_pair, keys[s], s, tokens)
            weights[s * tokens : (s + 1) * tokens, h * tokens : (h + 2) * tokens] = p.astype(BF16)
    grad = lax.dot_general(weights[...], g_all, NN, preferred_element_type=F32).astype(BF16)
    for s in range(n):
        out_ref[s] = grad[s * tokens : (s + 1) * tokens]


def slope_kernel(n, members, tokens, meta, q_ref, g_ref, o_ref, norm_ref, *rest):
    keys, values = rest[:n], rest[n : 2 * n]
    dq_ref, dk_ref, slopes, deltas = rest[2 * n :]
    q_all = jnp.concatenate([q_ref[0, :, h * HD : (h + 1) * HD] for h in range(members)], axis=0)
    for h in range(members):
        prod = (
            g_ref[0, :, h * HD : (h + 1) * HD].astype(F32)
            * o_ref[0, :, h * HD : (h + 1) * HD].astype(F32)
        )
        deltas[0, h : h + 1, :] = jnp.sum(prod.T, axis=0, keepdims=True)
    for h in range(0, members, 2):
        q_pair = pair_of(q_ref, h)
        g_pair = pair_of(g_ref, h)
        norm_pair = rows_of(norm_ref, h)
        delta_pair = rows_of(deltas, h)
        for s in range(n):
            p = probability(meta, q_pair, norm_pair, keys[s], s, tokens)
            through = lax.dot_general(values[s][0], g_pair, NT, preferred_element_type=F32)
            slopes[s * tokens : (s + 1) * tokens, h * tokens : (h + 2) * tokens] = (
                p * (through - delta_pair)
            ).astype(BF16)
    grad = lax.dot_general(slopes[...], q_all, NN, preferred_element_type=F32).astype(BF16)
    for s in range(n):
        dk_ref[s] = grad[s * tokens : (s + 1) * tokens]
    keys_t = jnp.concatenate([keys[s][0] for s in range(n)], axis=0).T
    dq_t = lax.dot_general(keys_t, slopes[...], NN, preferred_element_type=F32) * (HD ** (-0.5))
    for h in range(members):
        dq_ref[0, :, h * HD : (h + 1) * HD] = dq_t[:, h * tokens : (h + 1) * tokens].T.astype(BF16)


def shards(
    hidden,
    query_heads,
    key_heads,
    value_heads,
    attention_out,
    output_grad,
    log_norm,
    block_order,
    value_weight,
):
    tokens = query_heads.shape[1]
    groups = key_heads.shape[2] // HD
    members = HQ // KVH
    n = lax.axis_size("ctx")
    dp = lax.axis_size("dp")
    tp = lax.axis_size("tp")
    rank = lax.axis_index("ctx")
    wide = members * HD
    meta = jnp.concatenate([rank[None].astype(jnp.int32), block_order])

    keys = [key_heads] + [swap(key_heads, "ctx", s) for s in range(1, n)]
    values = [value_heads] + [swap(value_heads, "ctx", s) for s in range(1, n)]

    smem = pl.BlockSpec(memory_space=pltpu.SMEM)

    def value_terms(g):
        col = lambda i: (0, 0, g)
        return pl.pallas_call(
            lambda *refs: value_kernel(n, members, tokens, *refs),
            grid=(1,),
            in_specs=[
                smem,
                pl.BlockSpec((1, tokens, wide), col),
                pl.BlockSpec((1, tokens, wide), col),
                pl.BlockSpec((1, members, tokens), lambda i: (0, g, 0)),
            ]
            + [pl.BlockSpec((1, tokens, HD), col)] * n,
            out_specs=pl.BlockSpec((n, tokens, HD), lambda i: (0, 0, 0)),
            out_shape=jax.ShapeDtypeStruct((n, tokens, HD), BF16),
            scratch_shapes=[pltpu.VMEM((n * tokens, members * tokens), BF16)],
            name=f"value_terms_{g}",
        )(meta, query_heads, output_grad, log_norm, *keys)

    def reduce_ctx(x):
        bit = 1
        while bit < n:
            got = swap(x, "ctx", bit)
            got = got.reshape(n // (2 * bit), 2, bit, tokens, HD)[:, ::-1].reshape(x.shape)
            x = (x.astype(F32) + got.astype(F32)).astype(BF16)
            bit *= 2
        return x

    width = hidden.shape[2] // n
    split_dp = dp > 1 and is_pow2(dp) and width % dp == 0 and dp <= 4
    half = width // 2
    dp_rank = lax.axis_index("dp")
    low = dp_rank % 2
    held, _ = lax.optimization_barrier((hidden[0], (keys, values)))

    def columns(owner):
        start = owner * width
        if not split_dp:
            return lax.dynamic_slice_in_dim(held, start, width, 1)
        return jnp.concatenate(
            [
                lax.dynamic_slice_in_dim(held, start + (1 - low) * half, half, 1),
                lax.dynamic_slice_in_dim(held, start + low * half, half, 1),
            ],
            axis=1,
        )

    inputs = jnp.stack(
        [columns(rank)] + [swap(columns(rank ^ s), "ctx", s) for s in range(1, n)], axis=0
    )

    def reduce_dp(x):
        if not split_dp:
            return lax.psum(x, "dp").astype(F32)
        mine = (x[half:].astype(F32) + swap(x[:half], "dp", 1).astype(F32)).astype(BF16)
        bit = 2
        while bit < dp:
            mine = (mine.astype(F32) + swap(mine, "dp", bit).astype(F32)).astype(BF16)
            bit *= 2
        other = swap(mine, "dp", 1)
        return jnp.where(
            low == 0,
            jnp.concatenate([mine, other], axis=0),
            jnp.concatenate([other, mine], axis=0),
        ).astype(F32)

    reduced, weight_parts = [], []
    for g in range(groups):
        grad_g = reduce_ctx(value_terms(g))
        reduced.append(grad_g)
        part = jnp.einsum("std,ste->de", inputs, grad_g, preferred_element_type=F32).astype(BF16)
        weight_parts.append(reduce_dp(part))
    token_norm = (dp * n * tokens) ** (-0.5)
    weight_grad = jnp.concatenate(weight_parts, axis=1) * token_norm
    value_rows = jnp.concatenate([r[0] for r in reduced], axis=1)
    value_grad = value_rows[None]

    col = lambda g: (0, 0, g)
    query_grad, key_terms = pl.pallas_call(
        lambda *refs: slope_kernel(n, members, tokens, *refs),
        grid=(groups,),
        in_specs=[smem]
        + [pl.BlockSpec((1, tokens, wide), col)] * 3
        + [pl.BlockSpec((1, members, tokens), lambda g: (0, g, 0))]
        + [pl.BlockSpec((1, tokens, HD), col)] * (2 * n),
        out_specs=[
            pl.BlockSpec((1, tokens, wide), col),
            pl.BlockSpec((n, tokens, HD), col),
        ],
        out_shape=[
            jax.ShapeDtypeStruct((1, tokens, groups * wide), BF16),
            jax.ShapeDtypeStruct((n, tokens, groups * HD), BF16),
        ],
        scratch_shapes=[
            pltpu.VMEM((n * tokens, members * tokens), BF16),
            pltpu.VMEM((1, members, tokens), F32),
        ],
        name="slope_terms",
    )(meta, query_heads, output_grad, attention_out, log_norm, *keys, *values)
    own_key = key_terms[0].astype(F32)
    for s in range(1, n):
        own_key = own_key + swap(key_terms[s], "ctx", s).astype(F32)
    key_grad = (own_key * (HD ** (-0.5))).astype(BF16)[None]

    tp_rank = lax.axis_index("tp")
    span = value_weight.shape[0] // tp

    def hidden_terms(owner):
        rows = lax.dynamic_slice_in_dim(value_weight, owner * span, span, 0)
        return jnp.einsum("te,de->td", value_rows, rows, preferred_element_type=F32)

    received = [swap(hidden_terms(tp_rank ^ s).astype(BF16), "tp", s) for s in range(1, tp)]
    summed = hidden_terms(tp_rank)
    for r in received:
        summed = summed + r.astype(F32)
    hidden_grad = summed.astype(BF16)[None]
    return (query_grad, key_grad, value_grad, hidden_grad, weight_grad)


def solution(mesh):
    placed = (
        P("dp", "ctx", None),
        P("dp", "ctx", "tp"),
        P("dp", "ctx", "tp"),
        P("dp", "ctx", "tp"),
        P("dp", "ctx", "tp"),
        P("dp", "ctx", "tp"),
        P("dp", "tp", "ctx"),
        P(),
        P(None, "tp"),
    )
    return jax.shard_map(
        shards,
        mesh=mesh,
        in_specs=placed,
        out_specs=(
            P("dp", "ctx", "tp"),
            P("dp", "ctx", "tp"),
            P("dp", "ctx", "tp"),
            P("dp", "ctx", "tp"),
            P("ctx", "tp"),
        ),
        check_vma=False,
    )
```

```python
import jax
import jax.numpy as jnp
from jax import lax
from jax.experimental import pallas as pl
from jax.experimental.pallas import tpu as pltpu
from jax.sharding import PartitionSpec as P

HD = 128
HQ = 32
KVH = 4
F32 = jnp.float32
BF16 = jnp.bfloat16
NT = (((1,), (1,)), ((), ()))
NN = (((1,), (0,)), ((), ()))
TN = (((0,), (0,)), ((), ()))


def is_pow2(n):
    return n & (n - 1) == 0


def after(x, *deps):
    return lax.optimization_barrier((x, deps))[0]


def swap(x, axis, s):
    n = lax.axis_size(axis)
    return lax.ppermute(x, axis, [(i, i ^ s) for i in range(n)])


def probability(meta, q_pair, norm_pair, key_ref, s, tokens):
    rank = meta[0]
    block = tokens // 2
    lane = lax.broadcasted_iota(jnp.int32, (1, 2 * tokens), 1) % tokens
    q_first = jnp.where(lane < block, meta[1 + 2 * rank], meta[2 + 2 * rank])
    q_pos = q_first * block + lane % block
    owner = rank ^ s
    row = lax.broadcasted_iota(jnp.int32, (tokens, 1), 0)
    k_first = jnp.where(row < block, meta[1 + 2 * owner], meta[2 + 2 * owner])
    k_pos = k_first * block + row % block
    scores = lax.dot_general(key_ref[0], q_pair, NT, preferred_element_type=F32)
    shifted = scores * (HD ** (-0.5)) - norm_pair
    return jnp.exp(jnp.where(k_pos <= q_pos, shifted, -jnp.inf))


def pair_of(ref, h):
    return jnp.concatenate(
        [ref[0, :, h * HD : (h + 1) * HD], ref[0, :, (h + 1) * HD : (h + 2) * HD]], axis=0
    )


def rows_of(ref, h):
    return jnp.concatenate([ref[0, h : h + 1, :], ref[0, h + 1 : h + 2, :]], axis=1)


def value_kernel(n, members, tokens, meta, q_ref, g_ref, norm_ref, *rest):
    keys, out_ref, weights = rest[:n], rest[n], rest[n + 1]
    g_all = jnp.concatenate([g_ref[0, :, h * HD : (h + 1) * HD] for h in range(members)], axis=0)
    for h in range(0, members, 2):
        q_pair = pair_of(q_ref, h)
        norm_pair = rows_of(norm_ref, h)
        for s in range(n):
            p = probability(meta, q_pair, norm_pair, keys[s], s, tokens)
            weights[s * tokens : (s + 1) * tokens, h * tokens : (h + 2) * tokens] = p.astype(BF16)
    grad = lax.dot_general(weights[...], g_all, NN, preferred_element_type=F32).astype(BF16)
    for s in range(n):
        out_ref[meta[0] ^ s] = grad[s * tokens : (s + 1) * tokens]


def weight_kernel(n, half, meta, mine_ref, got_ref, *rest):
    inputs, (first_ref, second_ref, own_ref) = rest[:n], rest[n:]
    first = second = None
    for s in range(n):
        owner = meta[0] ^ s
        rows = (mine_ref[owner].astype(F32) + got_ref[owner].astype(F32)).astype(BF16)
        if s == 0:
            own_ref[...] = rows
        one = lax.dot_general(inputs[s][:, :half], rows, TN, preferred_element_type=F32)
        two = lax.dot_general(inputs[s][:, half:], rows, TN, preferred_element_type=F32)
        first = one if first is None else first + one
        second = two if second is None else second + two
    first_ref[...] = first.astype(BF16)
    second_ref[...] = second.astype(BF16)


def slope_kernel(n, members, tokens, meta, q_ref, g_ref, o_ref, norm_ref, *rest):
    keys, values = rest[:n], rest[n : 2 * n]
    dq_ref, dk_ref, slopes, deltas = rest[2 * n :]
    q_all = jnp.concatenate([q_ref[0, :, h * HD : (h + 1) * HD] for h in range(members)], axis=0)
    for h in range(members):
        prod = (
            g_ref[0, :, h * HD : (h + 1) * HD].astype(F32)
            * o_ref[0, :, h * HD : (h + 1) * HD].astype(F32)
        )
        deltas[0, h : h + 1, :] = jnp.sum(prod.T, axis=0, keepdims=True)
    for h in range(0, members, 2):
        q_pair = pair_of(q_ref, h)
        g_pair = pair_of(g_ref, h)
        norm_pair = rows_of(norm_ref, h)
        delta_pair = rows_of(deltas, h)
        for s in range(n):
            p = probability(meta, q_pair, norm_pair, keys[s], s, tokens)
            through = lax.dot_general(values[s][0], g_pair, NT, preferred_element_type=F32)
            slopes[s * tokens : (s + 1) * tokens, h * tokens : (h + 2) * tokens] = (
                p * (through - delta_pair)
            ).astype(BF16)
    grad = lax.dot_general(slopes[...], q_all, NN, preferred_element_type=F32).astype(BF16)
    for s in range(n):
        dk_ref[s] = grad[s * tokens : (s + 1) * tokens]
    keys_t = jnp.concatenate([keys[s][0] for s in range(n)], axis=0).T
    dq_t = lax.dot_general(keys_t, slopes[...], NN, preferred_element_type=F32) * (HD ** (-0.5))
    for h in range(members):
        dq_ref[0, :, h * HD : (h + 1) * HD] = dq_t[:, h * tokens : (h + 1) * tokens].T.astype(BF16)


def shards(
    hidden,
    query_heads,
    key_heads,
    value_heads,
    attention_out,
    output_grad,
    log_norm,
    block_order,
    value_weight,
):
    tokens = query_heads.shape[1]
    groups = key_heads.shape[2] // HD
    members = HQ // KVH
    n = lax.axis_size("ctx")
    dp = lax.axis_size("dp")
    tp = lax.axis_size("tp")
    rank = lax.axis_index("ctx")
    wide = members * HD
    meta = jnp.concatenate([rank[None].astype(jnp.int32), block_order])

    keys = [key_heads] + [swap(key_heads, "ctx", s) for s in range(1, n)]
    late_values = after(value_heads, keys)
    values = [value_heads] + [swap(late_values, "ctx", s) for s in range(1, n)]

    smem = pl.BlockSpec(memory_space=pltpu.SMEM)

    def value_terms(g):
        col = lambda i: (0, 0, g)
        return pl.pallas_call(
            lambda *refs: value_kernel(n, members, tokens, *refs),
            grid=(1,),
            in_specs=[
                smem,
                pl.BlockSpec((1, tokens, wide), col),
                pl.BlockSpec((1, tokens, wide), col),
                pl.BlockSpec((1, members, tokens), lambda i: (0, g, 0)),
            ]
            + [pl.BlockSpec((1, tokens, HD), col)] * n,
            out_specs=pl.BlockSpec((n, tokens, HD), lambda i: (0, 0, 0)),
            out_shape=jax.ShapeDtypeStruct((n, tokens, HD), BF16),
            scratch_shapes=[pltpu.VMEM((n * tokens, members * tokens), BF16)],
            name=f"value_terms_{g}",
        )(meta, query_heads, output_grad, log_norm, *keys)

    width = hidden.shape[2] // n
    split_dp = dp > 1 and is_pow2(dp) and width % dp == 0 and dp <= 4
    half = width // 2
    dp_rank = lax.axis_index("dp")
    low = dp_rank % 2
    held = hidden[0]

    def columns(owner):
        start = owner * width
        if not split_dp:
            return lax.dynamic_slice_in_dim(held, start, width, 1)
        return jnp.concatenate(
            [
                lax.dynamic_slice_in_dim(held, start + (1 - low) * half, half, 1),
                lax.dynamic_slice_in_dim(held, start + low * half, half, 1),
            ],
            axis=1,
        )

    inputs = [columns(rank)] + [
        swap(after(columns(rank ^ s), keys), "ctx", s) for s in range(1, n)
    ]

    def slope_terms(g, order, outs):
        col = lambda i: (0, 0, g)
        held_outs = [pl.BlockSpec(memory_space=pl.ANY)] * len(outs)
        count = 5 + 2 * n

        def body(*refs):
            slope_kernel(n, members, tokens, *refs[:count], *refs[count + len(outs) :])

        return pl.pallas_call(
            body,
            grid=(1,),
            in_specs=[smem]
            + [pl.BlockSpec((1, tokens, wide), col)] * 3
            + [pl.BlockSpec((1, members, tokens), lambda i: (0, g, 0))]
            + [pl.BlockSpec((1, tokens, HD), col)] * (2 * n)
            + held_outs,
            out_specs=[
                pl.BlockSpec((1, tokens, wide), col),
                pl.BlockSpec((n, tokens, HD), col),
            ],
            out_shape=[
                jax.ShapeDtypeStruct((1, tokens, groups * wide), BF16),
                jax.ShapeDtypeStruct((n, tokens, groups * HD), BF16),
            ],
            input_output_aliases={count + i: i for i in range(len(outs))},
            scratch_shapes=[
                pltpu.VMEM((n * tokens, members * tokens), BF16),
                pltpu.VMEM((1, members, tokens), F32),
            ],
            name=f"slope_terms_{g}",
        )(order, query_heads, output_grad, attention_out, log_norm, *keys, *values, *outs)

    def weight_terms(g, x, got):
        return pl.pallas_call(
            lambda *refs: weight_kernel(n, half, *refs),
            in_specs=[smem] + [pl.BlockSpec(memory_space=pltpu.VMEM)] * (2 + n),
            out_shape=[
                jax.ShapeDtypeStruct((half, HD), BF16),
                jax.ShapeDtypeStruct((half, HD), BF16),
                jax.ShapeDtypeStruct((tokens, HD), BF16),
            ],
            name=f"weight_terms_{g}",
        )(meta, x, got, *inputs)

    sums = []
    for g in range(groups):
        sums.append(value_terms(g))
    outs = slope_terms(0, after(meta, sums[-1]), [])
    last = n // 2
    bit = 1
    while bit < last:
        got = [after(swap(x, "ctx", bit), outs[1]) for x in sums]
        sums = [(x.astype(F32) + y.astype(F32)).astype(BF16) for x, y in zip(sums, got)]
        bit *= 2
    got = [swap(x, "ctx", last) for x in sums]
    for g in range(1, groups):
        outs = slope_terms(g, after(meta, sums[-1]), outs)
    query_grad, key_terms = outs

    own_rows, firsts, seconds = [], [], []
    for g in range(groups):
        first, second, own = weight_terms(g, sums[g], after(got[g], key_terms))
        own_rows.append(own)
        firsts.append(first)
        seconds.append(second)
    value_rows = jnp.concatenate(own_rows, axis=1)
    value_grad = value_rows[None]

    late_terms = after(key_terms, seconds[-1])
    own_key = key_terms[0].astype(F32)
    for s in range(1, n):
        own_key = own_key + swap(late_terms[s], "ctx", s).astype(F32)
    key_grad = (own_key * (HD ** (-0.5))).astype(BF16)[None]

    tp_rank = lax.axis_index("tp")
    span = value_weight.shape[0] // tp

    def hidden_terms(owner):
        rows = lax.dynamic_slice_in_dim(value_weight, owner * span, span, 0)
        return jnp.einsum("te,de->td", value_rows, rows, preferred_element_type=F32)

    received = [swap(hidden_terms(tp_rank ^ s).astype(BF16), "tp", s) for s in range(1, tp)]
    summed = hidden_terms(tp_rank)
    for r in received:
        summed = summed + r.astype(F32)
    hidden_grad = summed.astype(BF16)[None]

    def reduce_dp(send, keep):
        if not split_dp:
            return lax.psum(jnp.concatenate([send, keep], axis=0), "dp").astype(F32)
        mine = (keep.astype(F32) + swap(send, "dp", 1).astype(F32)).astype(BF16)
        bit = 2
        while bit < dp:
            mine = (mine.astype(F32) + swap(mine, "dp", bit).astype(F32)).astype(BF16)
            bit *= 2
        other = after(swap(mine, "dp", 1), hidden_grad, key_grad)
        return jnp.where(
            low == 0,
            jnp.concatenate([mine, other], axis=0),
            jnp.concatenate([other, mine], axis=0),
        ).astype(F32)

    token_norm = (dp * n * tokens) ** (-0.5)
    weight_grad = (
        jnp.concatenate([reduce_dp(a, b) for a, b in zip(firsts, seconds)], axis=1) * token_norm
    )
    return (query_grad, key_grad, value_grad, hidden_grad, weight_grad)


def solution(mesh):
    placed = (
        P("dp", "ctx", None),
        P("dp", "ctx", "tp"),
        P("dp", "ctx", "tp"),
        P("dp", "ctx", "tp"),
        P("dp", "ctx", "tp"),
        P("dp", "ctx", "tp"),
        P("dp", "tp", "ctx"),
        P(),
        P(None, "tp"),
    )
    return jax.shard_map(
        shards,
        mesh=mesh,
        in_specs=placed,
        out_specs=(
            P("dp", "ctx", "tp"),
            P("dp", "ctx", "tp"),
            P("dp", "ctx", "tp"),
            P("dp", "ctx", "tp"),
            P("ctx", "tp"),
        ),
        check_vma=False,
    )
```

```python
import jax
import jax.numpy as jnp
from jax import lax
from jax.experimental import pallas as pl
from jax.experimental.pallas import tpu as pltpu
from jax.sharding import PartitionSpec as P


HD = 128
HQ = 32
KVH = 4
F32 = jnp.float32
BF16 = jnp.bfloat16
NT = (((1,), (1,)), ((), ()))
NN = (((1,), (0,)), ((), ()))


def is_pow2(n):
    return n & (n - 1) == 0


def after(x, *deps):
    return lax.optimization_barrier((x, deps))[0]


def swap(x, axis, s):
    n = lax.axis_size(axis)
    return lax.ppermute(x, axis, [(i, i ^ s) for i in range(n)])


def probability(meta, q_pair, norm_pair, key_ref, s, tokens):
    rank = meta[0]
    block = tokens // 2
    lane = lax.broadcasted_iota(jnp.int32, (1, 2 * tokens), 1) % tokens
    q_first = jnp.where(lane < block, meta[1 + 2 * rank], meta[2 + 2 * rank])
    q_pos = q_first * block + lane % block
    owner = rank ^ s
    row = lax.broadcasted_iota(jnp.int32, (tokens, 1), 0)
    k_first = jnp.where(row < block, meta[1 + 2 * owner], meta[2 + 2 * owner])
    k_pos = k_first * block + row % block
    scores = lax.dot_general(key_ref[0], q_pair, NT, preferred_element_type=F32)
    shifted = scores * (HD ** (-0.5)) - norm_pair
    return jnp.exp(jnp.where(k_pos <= q_pos, shifted, -jnp.inf))


def pair_of(ref, h):
    return jnp.concatenate(
        [ref[0, :, h * HD : (h + 1) * HD], ref[0, :, (h + 1) * HD : (h + 2) * HD]], axis=0
    )


def rows_of(ref, h):
    return jnp.concatenate([ref[0, h : h + 1, :], ref[0, h + 1 : h + 2, :]], axis=1)


def value_kernel(n, members, tokens, meta, q_ref, g_ref, norm_ref, *rest):
    keys, out_ref, weights = rest[:n], rest[n], rest[n + 1]
    g_all = jnp.concatenate([g_ref[0, :, h * HD : (h + 1) * HD] for h in range(members)], axis=0)
    for h in range(0, members, 2):
        q_pair = pair_of(q_ref, h)
        norm_pair = rows_of(norm_ref, h)
        for s in range(n):
            p = probability(meta, q_pair, norm_pair, keys[s], s, tokens)
            weights[s * tokens : (s + 1) * tokens, h * tokens : (h + 2) * tokens] = p.astype(BF16)
    grad = lax.dot_general(weights[...], g_all, NN, preferred_element_type=F32).astype(BF16)
    for s in range(n):
        out_ref[meta[0] ^ s] = grad[s * tokens : (s + 1) * tokens]


def turn_kernel(n, tokens, meta, *refs):
    for s in range(n):
        start = pl.multiple_of((meta[0] ^ s) * tokens, tokens)
        refs[n][:, pl.ds(start, tokens)] = refs[s][...].T


def weight_kernel(n, half, tokens, meta, mine_ref, got_ref, turned, first_ref, second_ref, own_ref):
    rows = (mine_ref[...].astype(F32) + got_ref[...].astype(F32)).astype(BF16)
    owner = meta[0]
    own_ref[...] = (mine_ref[owner].astype(F32) + got_ref[owner].astype(F32)).astype(BF16)
    rows = rows.reshape(n * tokens, HD)
    first_ref[...] = lax.dot_general(
        turned[:half], rows, NN, preferred_element_type=F32
    ).astype(BF16)
    second_ref[...] = lax.dot_general(
        turned[half:], rows, NN, preferred_element_type=F32
    ).astype(BF16)


def slope_kernel(n, members, tokens, meta, q_ref, g_ref, o_ref, norm_ref, *rest):
    keys, values = rest[:n], rest[n : 2 * n]
    dq_ref, dk_ref, slopes, deltas = rest[2 * n :]
    q_all = jnp.concatenate([q_ref[0, :, h * HD : (h + 1) * HD] for h in range(members)], axis=0)
    for h in range(members):
        prod = (
            g_ref[0, :, h * HD : (h + 1) * HD].astype(F32)
            * o_ref[0, :, h * HD : (h + 1) * HD].astype(F32)
        )
        deltas[0, h : h + 1, :] = jnp.sum(prod.T, axis=0, keepdims=True)
    for h in range(0, members, 2):
        q_pair = pair_of(q_ref, h)
        g_pair = pair_of(g_ref, h)
        norm_pair = rows_of(norm_ref, h)
        delta_pair = rows_of(deltas, h)
        for s in range(n):
            p = probability(meta, q_pair, norm_pair, keys[s], s, tokens)
            through = lax.dot_general(values[s][0], g_pair, NT, preferred_element_type=F32)
            slopes[s * tokens : (s + 1) * tokens, h * tokens : (h + 2) * tokens] = (
                p * (through - delta_pair)
            ).astype(BF16)
    grad = lax.dot_general(slopes[...], q_all, NN, preferred_element_type=F32).astype(BF16)
    for s in range(n):
        dk_ref[s] = grad[s * tokens : (s + 1) * tokens]
    keys_t = jnp.concatenate([keys[s][0] for s in range(n)], axis=0).T
    dq_t = lax.dot_general(keys_t, slopes[...], NN, preferred_element_type=F32) * (HD ** (-0.5))
    for h in range(members):
        dq_ref[0, :, h * HD : (h + 1) * HD] = dq_t[:, h * tokens : (h + 1) * tokens].T.astype(BF16)


def shards(
    hidden,
    query_heads,
    key_heads,
    value_heads,
    attention_out,
    output_grad,
    log_norm,
    block_order,
    value_weight,
):
    tokens = query_heads.shape[1]
    groups = key_heads.shape[2] // HD
    members = HQ // KVH
    n = lax.axis_size("ctx")
    dp = lax.axis_size("dp")
    tp = lax.axis_size("tp")
    rank = lax.axis_index("ctx")
    wide = members * HD
    meta = jnp.concatenate([rank[None].astype(jnp.int32), block_order])

    keys = [key_heads] + [swap(key_heads, "ctx", s) for s in range(1, n)]
    values = [value_heads] + [swap(value_heads, "ctx", s) for s in range(1, n)]

    smem = pl.BlockSpec(memory_space=pltpu.SMEM)

    def value_terms(g):
        col = lambda i: (0, 0, g)
        return pl.pallas_call(
            lambda *refs: value_kernel(n, members, tokens, *refs),
            grid=(1,),
            in_specs=[
                smem,
                pl.BlockSpec((1, tokens, wide), col),
                pl.BlockSpec((1, tokens, wide), col),
                pl.BlockSpec((1, members, tokens), lambda i: (0, g, 0)),
            ]
            + [pl.BlockSpec((1, tokens, HD), col)] * n,
            out_specs=pl.BlockSpec((n, tokens, HD), lambda i: (0, 0, 0)),
            out_shape=jax.ShapeDtypeStruct((n, tokens, HD), BF16),
            scratch_shapes=[pltpu.VMEM((n * tokens, members * tokens), BF16)],
        )(meta, query_heads, output_grad, log_norm, *keys)

    width = hidden.shape[2] // n
    split_dp = dp > 1 and is_pow2(dp) and width % dp == 0 and dp <= 4
    half = width // 2
    dp_rank = lax.axis_index("dp")
    low = dp_rank % 2
    held = hidden[0]

    def columns(owner):
        start = owner * width
        if not split_dp:
            return lax.dynamic_slice_in_dim(held, start, width, 1)
        return jnp.concatenate(
            [
                lax.dynamic_slice_in_dim(held, start + (1 - low) * half, half, 1),
                lax.dynamic_slice_in_dim(held, start + low * half, half, 1),
            ],
            axis=1,
        )

    inputs = [columns(rank)]
    for s in range(1, n):
        piece = columns(rank ^ s)
        inputs.append(swap(piece, "ctx", s))

    def slope_terms(g, order, outs):
        col = lambda i: (0, 0, g)
        held_outs = [pl.BlockSpec(memory_space=pl.ANY)] * len(outs)
        count = 5 + 2 * n

        def body(*refs):
            slope_kernel(n, members, tokens, *refs[:count], *refs[count + len(outs) :])

        return pl.pallas_call(
            body,
            grid=(1,),
            in_specs=[smem]
            + [pl.BlockSpec((1, tokens, wide), col)] * 3
            + [pl.BlockSpec((1, members, tokens), lambda i: (0, g, 0))]
            + [pl.BlockSpec((1, tokens, HD), col)] * (2 * n)
            + held_outs,
            out_specs=[
                pl.BlockSpec((1, tokens, wide), col),
                pl.BlockSpec((n, tokens, HD), col),
            ],
            out_shape=[
                jax.ShapeDtypeStruct((1, tokens, groups * wide), BF16),
                jax.ShapeDtypeStruct((n, tokens, groups * HD), BF16),
            ],
            input_output_aliases={count + i: i for i in range(len(outs))},
            scratch_shapes=[
                pltpu.VMEM((n * tokens, members * tokens), BF16),
                pltpu.VMEM((1, members, tokens), F32),
            ],
        )(order, query_heads, output_grad, attention_out, log_norm, *keys, *values, *outs)

    vmem = pl.BlockSpec(memory_space=pltpu.VMEM)

    def weight_terms(x, got, turned):
        return pl.pallas_call(
            lambda *refs: weight_kernel(n, half, tokens, *refs),
            in_specs=[smem] + [vmem] * 3,
            out_shape=[
                jax.ShapeDtypeStruct((half, HD), BF16),
                jax.ShapeDtypeStruct((half, HD), BF16),
                jax.ShapeDtypeStruct((tokens, HD), BF16),
            ],
        )(meta, x, got, turned)

    sums = []
    for g in range(groups):
        sums.append(value_terms(g))
    outs = slope_terms(0, after(meta, sums[-1]), [])
    last = n // 2
    bit = 1
    while bit < last:
        got = []
        for g in range(groups):
            got.append(after(swap(sums[g], "ctx", bit), outs[1]))
        sums = [(x.astype(F32) + y.astype(F32)).astype(BF16) for x, y in zip(sums, got)]
        bit *= 2
    got = []
    for g in range(groups):
        got.append(swap(sums[g], "ctx", last))
    for g in range(1, groups):
        outs = slope_terms(g, after(meta, sums[-1]), outs)
    query_grad, key_terms = outs
    turned = pl.pallas_call(
        lambda *refs: turn_kernel(n, tokens, *refs),
        in_specs=[smem] + [vmem] * n,
        out_specs=vmem,
        out_shape=jax.ShapeDtypeStruct((width, n * tokens), BF16),
        name="turn",
    )(after(meta, key_terms), *inputs)

    own_rows, firsts, seconds = [], [], []
    for g in range(groups):
        first, second, own = weight_terms(sums[g], after(got[g], turned), turned)
        own_rows.append(own)
        firsts.append(first)
        seconds.append(second)
    value_rows = jnp.concatenate(own_rows, axis=1)
    value_grad = value_rows[None]

    mines = []
    for g in range(groups):
        if split_dp:
            part = swap(firsts[g], "dp", 1)
            mines.append((seconds[g].astype(F32) + part.astype(F32)).astype(BF16))
        else:
            mines.append(seconds[g])

    late_terms = after(key_terms, mines[-1])
    own_key = key_terms[0].astype(F32)
    for s in range(1, n):
        own_key = own_key + swap(late_terms[s], "ctx", s).astype(F32)
    key_grad = (own_key * (HD ** (-0.5))).astype(BF16)[None]

    tp_rank = lax.axis_index("tp")
    span = value_weight.shape[0] // tp

    def hidden_terms(owner):
        rows = lax.dynamic_slice_in_dim(value_weight, owner * span, span, 0)
        return jnp.einsum("te,de->td", late_rows, rows, preferred_element_type=F32)

    late_rows = after(value_rows, mines[0])

    received = [swap(hidden_terms(tp_rank ^ s).astype(BF16), "tp", s) for s in range(1, tp)]
    summed = hidden_terms(tp_rank)
    for r in received:
        summed = summed + r.astype(F32)
    hidden_grad = summed.astype(BF16)[None]

    def finish_dp(g):
        if not split_dp:
            return lax.psum(jnp.concatenate([firsts[g], mines[g]], axis=0), "dp").astype(F32)
        mine, bit = mines[g], 2
        while bit < dp:
            mine = (mine.astype(F32) + swap(mine, "dp", bit).astype(F32)).astype(BF16)
            bit *= 2
        other = swap(mine, "dp", 1)
        if g == groups - 1:
            other = after(other, hidden_grad, key_grad)
        return jnp.where(
            low == 0,
            jnp.concatenate([mine, other], axis=0),
            jnp.concatenate([other, mine], axis=0),
        ).astype(F32)

    token_norm = (dp * n * tokens) ** (-0.5)
    weight_grad = (
        jnp.concatenate([finish_dp(g) for g in range(groups)], axis=1) * token_norm
    )
    return (query_grad, key_grad, value_grad, hidden_grad, weight_grad)


def solution(mesh):
    placed = (
        P("dp", "ctx", None),
        P("dp", "ctx", "tp"),
        P("dp", "ctx", "tp"),
        P("dp", "ctx", "tp"),
        P("dp", "ctx", "tp"),
        P("dp", "ctx", "tp"),
        P("dp", "tp", "ctx"),
        P(),
        P(None, "tp"),
    )
    return jax.shard_map(
        shards,
        mesh=mesh,
        in_specs=placed,
        out_specs=(
            P("dp", "ctx", "tp"),
            P("dp", "ctx", "tp"),
            P("dp", "ctx", "tp"),
            P("dp", "ctx", "tp"),
            P("ctx", "tp"),
        ),
        check_vma=False,
    )
```

```python
import jax
import jax.numpy as jnp
from jax import lax
from jax.experimental import pallas as pl
from jax.experimental.pallas import tpu as pltpu
from jax.sharding import PartitionSpec as P


HD = 128
HQ = 32
KVH = 4
F32 = jnp.float32
BF16 = jnp.bfloat16
NT = (((1,), (1,)), ((), ()))
NN = (((1,), (0,)), ((), ()))


def is_pow2(n):
    return n & (n - 1) == 0


def after(x, *deps):
    return lax.optimization_barrier((x, deps))[0]


def swap(x, axis, s):
    n = lax.axis_size(axis)
    return lax.ppermute(x, axis, [(i, i ^ s) for i in range(n)])


def probability(meta, q_pair, norm_pair, key_ref, s, tokens):
    rank = meta[0]
    block = tokens // 2
    lane = lax.broadcasted_iota(jnp.int32, (1, 2 * tokens), 1) % tokens
    q_first = jnp.where(lane < block, meta[1 + 2 * rank], meta[2 + 2 * rank])
    q_pos = q_first * block + lane % block
    owner = rank ^ s
    row = lax.broadcasted_iota(jnp.int32, (tokens, 1), 0)
    k_first = jnp.where(row < block, meta[1 + 2 * owner], meta[2 + 2 * owner])
    k_pos = k_first * block + row % block
    scores = lax.dot_general(key_ref[0], q_pair, NT, preferred_element_type=F32)
    shifted = scores * (HD ** (-0.5)) - norm_pair
    return jnp.exp(jnp.where(k_pos <= q_pos, shifted, -jnp.inf))


def pair_of(ref, h):
    return jnp.concatenate(
        [ref[0, :, h * HD : (h + 1) * HD], ref[0, :, (h + 1) * HD : (h + 2) * HD]], axis=0
    )


def rows_of(ref, h):
    return jnp.concatenate([ref[0, h : h + 1, :], ref[0, h + 1 : h + 2, :]], axis=1)


def value_kernel(n, members, tokens, meta, q_ref, g_ref, norm_ref, *rest):
    keys, out_ref, weights = rest[:n], rest[n], rest[n + 1]
    g_all = jnp.concatenate([g_ref[0, :, h * HD : (h + 1) * HD] for h in range(members)], axis=0)
    for h in range(0, members, 2):
        q_pair = pair_of(q_ref, h)
        norm_pair = rows_of(norm_ref, h)
        for s in range(n):
            p = probability(meta, q_pair, norm_pair, keys[s], s, tokens)
            weights[s * tokens : (s + 1) * tokens, h * tokens : (h + 2) * tokens] = p.astype(BF16)
    grad = lax.dot_general(weights[...], g_all, NN, preferred_element_type=F32).astype(BF16)
    for s in range(n):
        out_ref[meta[0] ^ s] = grad[s * tokens : (s + 1) * tokens]


def turn_kernel(n, tokens, meta, *refs):
    for s in range(n):
        start = pl.multiple_of((meta[0] ^ s) * tokens, tokens)
        refs[n][:, pl.ds(start, tokens)] = refs[s][...].T


def weight_kernel(n, half, tokens, meta, mine_ref, got_ref, turned, first_ref, second_ref, own_ref):
    rows = (mine_ref[...].astype(F32) + got_ref[...].astype(F32)).astype(BF16)
    owner = meta[0]
    own_ref[...] = (mine_ref[owner].astype(F32) + got_ref[owner].astype(F32)).astype(BF16)
    rows = rows.reshape(n * tokens, HD)
    first_ref[...] = lax.dot_general(
        turned[:half], rows, NN, preferred_element_type=F32
    ).astype(BF16)
    second_ref[...] = lax.dot_general(
        turned[half:], rows, NN, preferred_element_type=F32
    ).astype(BF16)


def slope_kernel(n, members, tokens, meta, q_ref, g_ref, o_ref, norm_ref, *rest):
    keys, values = rest[:n], rest[n : 2 * n]
    dq_ref, dk_ref, slopes, deltas = rest[2 * n :]
    q_all = jnp.concatenate([q_ref[0, :, h * HD : (h + 1) * HD] for h in range(members)], axis=0)
    for h in range(members):
        prod = (
            g_ref[0, :, h * HD : (h + 1) * HD].astype(F32)
            * o_ref[0, :, h * HD : (h + 1) * HD].astype(F32)
        )
        deltas[0, h : h + 1, :] = jnp.sum(prod.T, axis=0, keepdims=True)
    for h in range(0, members, 2):
        q_pair = pair_of(q_ref, h)
        g_pair = pair_of(g_ref, h)
        norm_pair = rows_of(norm_ref, h)
        delta_pair = rows_of(deltas, h)
        for s in range(n):
            p = probability(meta, q_pair, norm_pair, keys[s], s, tokens)
            through = lax.dot_general(values[s][0], g_pair, NT, preferred_element_type=F32)
            slopes[s * tokens : (s + 1) * tokens, h * tokens : (h + 2) * tokens] = (
                p * (through - delta_pair)
            ).astype(BF16)
    grad = lax.dot_general(slopes[...], q_all, NN, preferred_element_type=F32).astype(BF16)
    for s in range(n):
        dk_ref[s] = grad[s * tokens : (s + 1) * tokens]
    keys_t = jnp.concatenate([keys[s][0] for s in range(n)], axis=0).T
    dq_t = lax.dot_general(keys_t, slopes[...], NN, preferred_element_type=F32) * (HD ** (-0.5))
    for h in range(members):
        dq_ref[0, :, h * HD : (h + 1) * HD] = dq_t[:, h * tokens : (h + 1) * tokens].T.astype(BF16)


def shards(
    hidden,
    query_heads,
    key_heads,
    value_heads,
    attention_out,
    output_grad,
    log_norm,
    block_order,
    value_weight,
):
    tokens = query_heads.shape[1]
    groups = key_heads.shape[2] // HD
    members = HQ // KVH
    n = lax.axis_size("ctx")
    dp = lax.axis_size("dp")
    tp = lax.axis_size("tp")
    rank = lax.axis_index("ctx")
    wide = members * HD
    meta = jnp.concatenate([rank[None].astype(jnp.int32), block_order])

    keys = [key_heads] + [swap(key_heads, "ctx", s) for s in range(1, n)]
    values = [value_heads] + [swap(value_heads, "ctx", s) for s in range(1, n)]

    smem = pl.BlockSpec(memory_space=pltpu.SMEM)

    def value_terms(g):
        col = lambda i: (0, 0, g)
        return pl.pallas_call(
            lambda *refs: value_kernel(n, members, tokens, *refs),
            grid=(1,),
            in_specs=[
                smem,
                pl.BlockSpec((1, tokens, wide), col),
                pl.BlockSpec((1, tokens, wide), col),
                pl.BlockSpec((1, members, tokens), lambda i: (0, g, 0)),
            ]
            + [pl.BlockSpec((1, tokens, HD), col)] * n,
            out_specs=pl.BlockSpec((n, tokens, HD), lambda i: (0, 0, 0)),
            out_shape=jax.ShapeDtypeStruct((n, tokens, HD), BF16),
            scratch_shapes=[pltpu.VMEM((n * tokens, members * tokens), BF16)],
        )(meta, query_heads, output_grad, log_norm, *keys)

    width = hidden.shape[2] // n
    split_dp = dp > 1 and is_pow2(dp) and width % dp == 0 and dp <= 4
    half = width // 2
    dp_rank = lax.axis_index("dp")
    low = dp_rank % 2
    held = hidden[0]

    def columns(owner):
        start = owner * width
        if not split_dp:
            return lax.dynamic_slice_in_dim(held, start, width, 1)
        return jnp.concatenate(
            [
                lax.dynamic_slice_in_dim(held, start + (1 - low) * half, half, 1),
                lax.dynamic_slice_in_dim(held, start + low * half, half, 1),
            ],
            axis=1,
        )

    inputs = [columns(rank)]
    for s in range(1, n):
        piece = columns(rank ^ s)
        inputs.append(swap(piece, "ctx", s))

    def slope_terms(g, order, outs):
        col = lambda i: (0, 0, g)
        held_outs = [pl.BlockSpec(memory_space=pl.ANY)] * len(outs)
        count = 5 + 2 * n

        def body(*refs):
            slope_kernel(n, members, tokens, *refs[:count], *refs[count + len(outs) :])

        return pl.pallas_call(
            body,
            grid=(1,),
            in_specs=[smem]
            + [pl.BlockSpec((1, tokens, wide), col)] * 3
            + [pl.BlockSpec((1, members, tokens), lambda i: (0, g, 0))]
            + [pl.BlockSpec((1, tokens, HD), col)] * (2 * n)
            + held_outs,
            out_specs=[
                pl.BlockSpec((1, tokens, wide), col),
                pl.BlockSpec((n, tokens, HD), col),
            ],
            out_shape=[
                jax.ShapeDtypeStruct((1, tokens, groups * wide), BF16),
                jax.ShapeDtypeStruct((n, tokens, groups * HD), BF16),
            ],
            input_output_aliases={count + i: i for i in range(len(outs))},
            scratch_shapes=[
                pltpu.VMEM((n * tokens, members * tokens), BF16),
                pltpu.VMEM((1, members, tokens), F32),
            ],
        )(order, query_heads, output_grad, attention_out, log_norm, *keys, *values, *outs)

    vmem = pl.BlockSpec(memory_space=pltpu.VMEM)

    def weight_terms(x, got, turned):
        return pl.pallas_call(
            lambda *refs: weight_kernel(n, half, tokens, *refs),
            in_specs=[smem] + [vmem] * 3,
            out_shape=[
                jax.ShapeDtypeStruct((half, HD), BF16),
                jax.ShapeDtypeStruct((half, HD), BF16),
                jax.ShapeDtypeStruct((tokens, HD), BF16),
            ],
        )(meta, x, got, turned)

    sums = []
    for g in range(groups):
        sums.append(value_terms(g))
    outs = slope_terms(0, after(meta, sums[-1]), [])
    last = n // 2
    bit = 1
    while bit < last:
        got = []
        for g in range(groups):
            got.append(after(swap(sums[g], "ctx", bit), outs[1]))
        sums = [(x.astype(F32) + y.astype(F32)).astype(BF16) for x, y in zip(sums, got)]
        bit *= 2
    got = []
    for g in range(groups):
        got.append(swap(sums[g], "ctx", last))
    for g in range(1, groups):
        outs = slope_terms(g, after(meta, sums[-1]), outs)
    query_grad, key_terms = outs
    turned = pl.pallas_call(
        lambda *refs: turn_kernel(n, tokens, *refs),
        in_specs=[smem] + [vmem] * n,
        out_specs=vmem,
        out_shape=jax.ShapeDtypeStruct((width, n * tokens), BF16),
        name="turn",
    )(after(meta, key_terms), *inputs)

    own_rows, firsts, seconds = [], [], []
    for g in range(groups):
        first, second, own = weight_terms(sums[g], after(got[g], turned), turned)
        own_rows.append(own)
        firsts.append(first)
        seconds.append(second)
    value_rows = jnp.concatenate(own_rows, axis=1)
    value_grad = value_rows[None]

    mines = []
    for g in range(groups):
        if split_dp:
            part = swap(firsts[g], "dp", 1)
            mines.append((seconds[g].astype(F32) + part.astype(F32)).astype(BF16))
        else:
            mines.append(seconds[g])

    late_terms = after(key_terms, mines[-1])
    own_key = key_terms[0].astype(F32)
    for s in range(1, n):
        part = swap(late_terms[s], "ctx", s)
        own_key = own_key + part.astype(F32)
    key_grad = (own_key * (HD ** (-0.5))).astype(BF16)[None]

    tp_rank = lax.axis_index("tp")
    span = value_weight.shape[0] // tp

    def hidden_terms(owner):
        rows = lax.dynamic_slice_in_dim(value_weight, owner * span, span, 0)
        return jnp.einsum("te,de->td", late_rows, rows, preferred_element_type=F32)

    late_rows = after(value_rows, mines[0])

    received = []
    for s in range(1, tp):
        part = hidden_terms(tp_rank ^ s).astype(BF16)
        received.append(swap(part, "tp", s))
    summed = hidden_terms(tp_rank)
    for r in received:
        summed = summed + r.astype(F32)
    hidden_grad = summed.astype(BF16)[None]

    def finish_dp(g):
        if not split_dp:
            return lax.psum(jnp.concatenate([firsts[g], mines[g]], axis=0), "dp").astype(F32)
        mine, bit = mines[g], 2
        while bit < dp:
            across = swap(mine, "dp", bit)
            mine = (mine.astype(F32) + across.astype(F32)).astype(BF16)
            bit *= 2
        other = swap(mine, "dp", 1)
        if g == groups - 1:
            other = after(other, hidden_grad, key_grad)
        return jnp.where(
            low == 0,
            jnp.concatenate([mine, other], axis=0),
            jnp.concatenate([other, mine], axis=0),
        ).astype(F32)

    token_norm = (dp * n * tokens) ** (-0.5)
    weight_grad = (
        jnp.concatenate([finish_dp(g) for g in range(groups)], axis=1) * token_norm
    )
    return (query_grad, key_grad, value_grad, hidden_grad, weight_grad)


def solution(mesh):
    placed = (
        P("dp", "ctx", None),
        P("dp", "ctx", "tp"),
        P("dp", "ctx", "tp"),
        P("dp", "ctx", "tp"),
        P("dp", "ctx", "tp"),
        P("dp", "ctx", "tp"),
        P("dp", "tp", "ctx"),
        P(),
        P(None, "tp"),
    )
    return jax.shard_map(
        shards,
        mesh=mesh,
        in_specs=placed,
        out_specs=(
            P("dp", "ctx", "tp"),
            P("dp", "ctx", "tp"),
            P("dp", "ctx", "tp"),
            P("dp", "ctx", "tp"),
            P("ctx", "tp"),
        ),
        check_vma=False,
    )
```
